32 devices in a mesh: fsdp: 4 (over y, x), width: 8 (over z, core).
Axes of the slice: x: 2, y: 2, z: 4, core: 2. Of those that a mesh axis runs over, the one named last changes fastest.
Arguments:
- train_gate: float32 [4096, 11008], P('fsdp', 'width'), may hold values from -0.125 to 0.125
- drift_gate: float32 [4096, 11008], P('fsdp', 'width'), may hold values from -0.09375 to 0.09375
- spread_gate: float32 [4096, 11008], P('fsdp', 'width'), may hold values from -0.09375 to 0.09375
- train_up: float32 [4096, 11008], P('fsdp', 'width'), may hold values from -0.125 to 0.125
- drift_up: float32 [4096, 11008], P('fsdp', 'width'), may hold values from -0.09375 to 0.09375
- spread_up: float32 [4096, 11008], P('fsdp', 'width'), may hold values from -0.09375 to 0.09375
- norm_train: float32 [4096], P(('fsdp', 'width')), may hold values from 0.25 to 1.75
- norm_step: float32 [4096], P(('fsdp', 'width')), may hold values from -0.3 to 0.3
Outputs:
- serving_gate: bfloat16 [4096, 11008], P(None, 'width')
- serving_up: bfloat16 [4096, 11008], P(None, 'width')
- scale_gate: float32 [11008], P('width')
- scale_up: float32 [11008], P('width')
- serve_norm: bfloat16 [4096], replicated
- whole_gate: float32 [4096, 11008], P('fsdp', 'width')
- whole_up: float32 [4096, 11008], P('fsdp', 'width')
The draws below stay inside these ranges and needn't reach their ends.
All inputs are finite; a program needn't handle non-finite values.
Results may differ from the reference program's by a relative error of at most 0.0004.
Values may be sent and summed in bfloat16 or wider, within the bound.
A program may use at most 128 MiB of HBM per device.

```python
import jax
import jax.numpy as jnp
from jax import lax

D_MODEL = 4096
D_INNER = 11008


def strengthened(entries, key, source, target, shards_of, factor):
    def block_of(axis_at):
        return (jnp.arange(entries.shape[axis_at]) // (entries.shape[axis_at] // shards_of)).reshape((-1,) + (1,) * (entries.ndim - 1 - axis_at))

    one_side = jax.random.permutation(key, shards_of)[block_of(target)]
    other_side = (block_of(target) + shards_of // 2) % shards_of
    return jnp.where((block_of(source) == one_side) | (block_of(source) == other_side), factor * entries, entries)


def level_of(own_key, dims, split, smallest, largest):
    loudness = 1.0
    for position, parts in split:
        draws = jax.random.uniform(jax.random.fold_in(jax.random.fold_in(own_key, 6), position), (parts,), jnp.float32, smallest / len(split), largest / len(split))
        loudness = loudness * jnp.repeat(jnp.exp(draws), dims[position] // parts).reshape((-1,) + (1,) * (len(dims) - 1 - position))
    return loudness


def gaussian(own_key, dims, width, reach, cuts=(), held_as=jnp.bfloat16):
    array = width * jax.random.normal(own_key, dims, jnp.float32)
    if cuts:
        array = array * level_of(own_key, dims, cuts, -0.22, 0.18)
    return jnp.clip(array, -reach, reach).astype(held_as)


def bell_draw_with(own_key, shape, spread, reach, split, heavy, dtype=jnp.bfloat16):
    values = spread * jax.random.normal(own_key, shape, jnp.float32)
    if split:
        values = values * level_of(own_key, shape, split, -0.22, 0.18)
    return jnp.clip(strengthened(values, jax.random.fold_in(own_key, 3), *heavy), -reach, reach).astype(dtype)


def setup_inputs(seed: int = 0) -> dict:
    seeds = jax.random.split(jax.random.key(seed), 9)
    return {
        "train_gate": bell_draw_with(seeds[0], (D_MODEL, D_INNER), D_MODEL ** -0.5, 0.125, ((0, 4), (1, 8)), (0, 1, 8, 2.0), jnp.float32),
        "drift_gate": gaussian(seeds[1], (D_MODEL, D_INNER), D_MODEL ** -0.5, 0.09375, ((0, 4), (1, 8)), jnp.float32),
        "spread_gate": gaussian(seeds[2], (D_MODEL, D_INNER), D_MODEL ** -0.5, 0.09375, ((0, 4), (1, 8)), jnp.float32),
        "train_up": bell_draw_with(seeds[3], (D_MODEL, D_INNER), D_MODEL ** -0.5, 0.125, ((0, 4), (1, 8)), (0, 1, 8, 2.0), jnp.float32),
        "drift_up": gaussian(seeds[4], (D_MODEL, D_INNER), D_MODEL ** -0.5, 0.09375, ((0, 4), (1, 8)), jnp.float32),
        "spread_up": gaussian(seeds[5], (D_MODEL, D_INNER), D_MODEL ** -0.5, 0.09375, ((0, 4), (1, 8)), jnp.float32),
        "norm_train": jnp.clip(1.0 + 0.15 * jax.random.normal(seeds[6], (D_MODEL,), jnp.float32), 0.25, 1.75),
        "norm_step": jnp.clip(jax.random.uniform(seeds[7], (D_MODEL,), jnp.float32, -0.3, 0.3) * level_of(seeds[7], (D_MODEL,), ((0, 32),), -0.4, 0.0), -0.3, 0.3),
    }


learn_rate = 0.3
hold_rate = 0.9

def reference(train_gate, drift_gate, spread_gate, train_up, drift_up, spread_up, norm_train, norm_step):
    hold_gate = hold_rate * drift_gate + spread_gate
    whole_gate = train_gate - learn_rate * hold_gate
    hold_up = hold_rate * drift_up + spread_up
    whole_up = train_up - learn_rate * hold_up
    scale_gate = jnp.sqrt(lax.optimization_barrier(jnp.sum(whole_gate * whole_gate, axis=0)))
    serving_gate = (whole_gate / scale_gate).astype(jnp.bfloat16)
    scale_up = jnp.sqrt(lax.optimization_barrier(jnp.sum(whole_up * whole_up, axis=0)))
    serving_up = (whole_up / scale_up).astype(jnp.bfloat16)
    serve_norm = (norm_train + norm_step).astype(jnp.bfloat16)
    return (serving_gate, serving_up, scale_gate, scale_up, serve_norm, whole_gate, whole_up)
```

```python
import functools

import jax
import jax.numpy as jnp
from jax import lax
from jax.experimental import pallas as pl
from jax.experimental.pallas import tpu as pltpu
from jax.sharding import PartitionSpec as P

learn_rate = 0.3
hold_rate = 0.9
LANES = 128
SUB = 16
MESH = pl.DeviceIdType.MESH


def ring_order(n):
    side = int(round(n**0.5))
    if side * side != n or side % 2:
        return list(range(n))
    walk = [y * side for y in range(side)]
    for y in reversed(range(side)):
        columns = range(1, side) if (side - 1 - y) % 2 == 0 else reversed(range(1, side))
        walk += [y * side + x for x in columns]
    return walk


def pick(table, index):
    value = jnp.int32(table[0])
    for k in range(1, len(table)):
        value = jnp.where(index == k, jnp.int32(table[k]), value)
    return value


def groups_of(columns):
    first = min(2 * LANES, columns // 2 // LANES * LANES)
    return [(0, 0, first), (0, first, columns - first), (1, 0, columns)]


def gather_kernel(n, w, order, names, *refs):
    (tg, dg, sg, tu, du, su, nt, ns) = refs[:8]
    (out_g, out_u, whole_g, whole_u, scale_out, norm_out) = refs[8:14]
    (tv, dv, sv, nv, sums, q, norm_buf) = refs[14:21]
    (in_sem, put_sem, sum_send, sum_recv, ring_send, ring_recv, nf_send, nf_recv, nw_send, nw_recv) = refs[21:]
    f_axis, w_axis = names
    columns, rows = tg.shape
    groups = groups_of(columns)
    args = ((tg, dg, sg), (tu, du, su))
    outs, wholes = (out_g, out_u), (whole_g, whole_u)
    me = lax.axis_index(f_axis)
    mw = lax.axis_index(w_axis)
    half_ring = n // 2
    at = {d: i for i, d in enumerate(order)}
    right = pick([order[(at[d] + 1) % n] for d in range(n)], me)
    left = pick([order[(at[d] - 1) % n] for d in range(n)], me)

    loads = []
    for g, (m, c0, cn) in enumerate(groups):
        for k, buf in enumerate((tv, dv, sv)):
            copy = pltpu.make_async_copy(
                args[m][k].at[pl.ds(c0, cn)], buf.at[m, pl.ds(c0, cn)], in_sem.at[g, k]
            )
            copy.start()
            loads.append(copy)

    barrier = pltpu.get_barrier_semaphore()
    for k in range(1, n):
        pl.semaphore_signal(
            barrier, inc=1, device_id={f_axis: lax.rem(me + k, n)}, device_id_type=MESH
        )
    for k in range(1, w):
        pl.semaphore_signal(
            barrier, inc=1, device_id={w_axis: lax.rem(mw + k, w)}, device_id_type=MESH
        )

    norm_buf[me, mw] = nt[0] + ns[0]
    q[...] = jnp.zeros_like(q)

    def blocks(c0, cn, body):
        full = cn // LANES

        @pl.loop(0, full)
        def _(b):
            body(pl.multiple_of(c0 + b * LANES, LANES), LANES)

        if cn % LANES:
            body(c0 + full * LANES, cn % LANES)

    def step_block(m, c, cn):
        for r in range(0, cn, SUB):
            at_rows = pl.ds(c + r, SUB)
            part = None
            for l in range(0, rows, LANES):
                lanes = pl.ds(l, LANES)
                hold = hold_rate * dv[m, at_rows, lanes] + sv[m, at_rows, lanes]
                new = tv[m, at_rows, lanes] - learn_rate * hold
                tv[m, at_rows, lanes] = new
                part = new * new if part is None else part + new * new
            q[pl.ds(r, SUB), :] = part
        sums[m, me, :, pl.ds(c, LANES)] = jnp.sum(q[...].T, axis=0, keepdims=True)

    def narrow_block(m, c, cn):
        lanes = pl.ds(c, LANES)
        total = sums[m, 0, :, lanes]
        for k in range(1, n):
            total = total + sums[m, k, :, lanes]
        scale = jnp.sqrt(total)
        scale_out[m, :, lanes] = scale
        q[...] = jnp.broadcast_to(scale, (LANES, LANES)).T
        for r in range(0, cn, SUB):
            at_rows = pl.ds(c + r, SUB)
            by = q[pl.ds(r, SUB), :]
            for l in range(0, rows, LANES):
                lanes = pl.ds(l, LANES)
                nv[m, at_rows, lanes] = (tv[m, at_rows, lanes] / by).astype(jnp.bfloat16)

    puts = []
    sends = []

    def exchange(g):
        m, c0, cn = groups[g]
        lanes = pl.ds(c0, -(-cn // LANES) * LANES)
        for k in range(1, n):
            copy = pltpu.make_async_remote_copy(
                src_ref=sums.at[m, me, :, lanes],
                dst_ref=sums.at[m, me, :, lanes],
                send_sem=sum_send.at[g, k],
                recv_sem=sum_recv.at[g, k],
                device_id={f_axis: lax.rem(me + k, n)},
                device_id_type=MESH,
            )
            copy.start()
            sends.append(copy)

    def exchanged(g):
        m, c0, cn = groups[g]
        lanes = pl.ds(c0, -(-cn // LANES) * LANES)
        for k in range(1, n):
            come = lax.rem(me - k + n, n)
            pltpu.make_async_remote_copy(
                src_ref=sums.at[m, come, :, lanes],
                dst_ref=sums.at[m, come, :, lanes],
                send_sem=sum_send.at[g, k],
                recv_sem=sum_recv.at[g, k],
                device_id={f_axis: come},
                device_id_type=MESH,
            ).wait_recv()

    def ring_part(g, s, way):
        _, c0, cn = groups[g]
        if s < half_ring - 1:
            return c0, cn
        cut = cn // (2 * SUB) * SUB
        return (c0, cut) if way == 0 else (c0 + cut, cn - cut)

    def origin(s, way):
        shift = -s if way == 0 else s
        return pick([order[(at[d] + shift) % n] for d in range(n)], me)

    def ring_copy(g, s, way, sent):
        m = groups[g][0]
        c0, cn = ring_part(g, s, way)
        block = origin(s if sent else s + 1, way)
        place = outs[m].at[pl.ds(c0, cn), pl.ds(pl.multiple_of(block * rows, LANES), rows)]
        source = nv.at[m, pl.ds(c0, cn)] if s == 0 and sent else place
        return pltpu.make_async_remote_copy(
            src_ref=source,
            dst_ref=place,
            send_sem=ring_send.at[g, s, way],
            recv_sem=ring_recv.at[g, s, way],
            device_id={f_axis: right if way == 0 else left},
            device_id_type=MESH,
        )

    def ring_start(g, s):
        for way in (0, 1):
            copy = ring_copy(g, s, way, True)
            copy.start()
            sends.append(copy)

    def norm_copy(axis, index, k, size, send, recv, place):
        return pltpu.make_async_remote_copy(
            src_ref=place,
            dst_ref=place,
            send_sem=send.at[k],
            recv_sem=recv.at[k],
            device_id={axis: lax.rem(index + k, size)},
            device_id_type=MESH,
        )

    for g, (m, c0, cn) in enumerate(groups):
        for copy in loads[3 * g : 3 * g + 3]:
            copy.wait()
        blocks(c0, cn, functools.partial(step_block, m))
        if g == 0:
            pl.semaphore_wait(barrier, n - 1 + w - 1)
        exchange(g)
        put = pltpu.make_async_copy(
            tv.at[m, pl.ds(c0, cn)], wholes[m].at[pl.ds(c0, cn)], put_sem.at[g, 0]
        )
        put.start()
        puts.append(put)
        if g == 0:
            for k in range(1, n):
                copy = norm_copy(f_axis, me, k, n, nf_send, nf_recv, norm_buf.at[me, mw])
                copy.start()
                sends.append(copy)
        exchanged(g)
        blocks(c0, cn, functools.partial(narrow_block, m))
        ring_start(g, 0)
        put = pltpu.make_async_copy(
            nv.at[m, pl.ds(c0, cn)],
            outs[m].at[pl.ds(c0, cn), pl.ds(pl.multiple_of(me * rows, LANES), rows)],
            put_sem.at[g, 1],
        )
        put.start()
        puts.append(put)

    for k in range(1, n):
        come = lax.rem(me - k + n, n)
        norm_copy(f_axis, me, k, n, nf_send, nf_recv, norm_buf.at[come, mw]).wait_recv()
    for k in range(1, w):
        copy = norm_copy(w_axis, mw, k, w, nw_send, nw_recv, norm_buf.at[:, mw])
        copy.start()
        sends.append(copy)
    for k in range(1, w):
        come = lax.rem(mw - k + w, w)
        norm_copy(w_axis, mw, k, w, nw_send, nw_recv, norm_buf.at[:, come]).wait_recv()
    norm_out[...] = norm_buf[...]

    for s in range(half_ring):
        for g in range(len(groups)):
            for way in (0, 1):
                ring_copy(g, s, way, False).wait_recv()
            if s + 1 < half_ring:
                ring_start(g, s + 1)
    for copy in sends:
        copy.wait_send()
    for copy in puts:
        copy.wait()


def solution(mesh):
    names = mesh.axis_names
    n, w = mesh.shape["fsdp"], mesh.shape["width"]
    order = ring_order(n)

    def shards(tg, dg, sg, tu, du, su, nt, ns):
        rows, columns = tg.shape
        padded = -(-columns // LANES) * LANES
        length = nt.shape[0]
        wide = -(-length // LANES) * LANES

        def line(x):
            return jnp.pad(x, (0, wide - length)).reshape(1, 1, wide)

        groups = len(groups_of(columns))
        hbm = pl.BlockSpec(memory_space=pl.ANY)
        vmem = pl.BlockSpec(memory_space=pltpu.VMEM)
        dma = pltpu.SemaphoreType.DMA
        sent = 3 * 2 * columns * rows * 2
        out_g, out_u, whole_g, whole_u, scales, norm = pl.pallas_call(
            functools.partial(gather_kernel, n, w, order, names),
            out_shape=(
                jax.ShapeDtypeStruct((columns, n * rows), jnp.bfloat16),
                jax.ShapeDtypeStruct((columns, n * rows), jnp.bfloat16),
                jax.ShapeDtypeStruct((columns, rows), jnp.float32),
                jax.ShapeDtypeStruct((columns, rows), jnp.float32),
                jax.ShapeDtypeStruct((2, 1, padded), jnp.float32),
                jax.ShapeDtypeStruct((n, w, 1, wide), jnp.float32),
            ),
            in_specs=[hbm] * 6 + [vmem] * 2,
            out_specs=[hbm] * 4 + [vmem] * 2,
            scratch_shapes=[
                pltpu.VMEM((2, columns, rows), jnp.float32),
                pltpu.VMEM((2, columns, rows), jnp.float32),
                pltpu.VMEM((2, columns, rows), jnp.float32),
                pltpu.VMEM((2, columns, rows), jnp.bfloat16),
                pltpu.VMEM((2, n, 1, padded), jnp.float32),
                pltpu.VMEM((LANES, LANES), jnp.float32),
                pltpu.VMEM((n, w, 1, wide), jnp.float32),
                dma((groups, 3)),
                dma((groups, 2)),
                dma((groups, n)),
                dma((groups, n)),
                dma((groups, n // 2, 2)),
                dma((groups, n // 2, 2)),
                dma((n,)),
                dma((n,)),
                dma((w,)),
                dma((w,)),
            ],
            compiler_params=pltpu.CompilerParams(
                collective_id=0, has_side_effects=True, vmem_limit_bytes=60 * 1024 * 1024
            ),
            cost_estimate=pl.CostEstimate(
                flops=20 * columns * rows, bytes_accessed=16 * sent, transcendentals=0
            ),
        )(tg.T, dg.T, sg.T, tu.T, du.T, su.T, line(nt), line(ns))
        serve_norm = norm[..., :length].reshape(n * w * length).astype(jnp.bfloat16)
        return (
            out_g.T,
            out_u.T,
            scales[0, 0, :columns],
            scales[1, 0, :columns],
            serve_norm,
            whole_g.T,
            whole_u.T,
        )

    split = P("fsdp", "width")
    flat = P(("fsdp", "width"))
    return jax.shard_map(
        shards,
        mesh=mesh,
        in_specs=(split,) * 6 + (flat,) * 2,
        out_specs=(P(None, "width"), P(None, "width"), P("width"), P("width"), P(), split, split),
        check_vma=False,
    )
```
